8 devices in a mesh: dp: 1 (over z), fsdp: 2 (over y), tp: 4 (over x, core).
Axes of the slice: x: 2, y: 2, z: 1, core: 2. Of those that a mesh axis runs over, the one named last changes fastest.
Arguments:
- hidden: bfloat16 [2048, 3072], P(('dp', 'fsdp', 'tp'))
- w_head: bfloat16 [3072, 128256], P('fsdp', 'tp')
- labels: int32 [2048], P(('dp', 'fsdp', 'tp'))
Outputs:
- output 1: float32 [1], P('dp')
- output 2: bfloat16 [2048, 3072], P(('dp', 'fsdp', 'tp'))
- output 3: bfloat16 [3072, 128256], P(('dp', 'fsdp'), 'tp')
All inputs are finite; a program needn't handle non-finite values.
Results may differ from the reference program's by a relative error of at most 0.001.
Values are sent between devices in bfloat16 or wider.
A program may use at most 1 GiB of HBM per device.

```python
import jax
import jax.numpy as jnp
from jax import lax

HIDDEN = 3072
VOCAB = 128256
TOKENS = 2048
ROW_BLOCK = 32
COL_ROWS = 256
VOCAB_SPLIT = 16


def setup_inputs(seed: int = 0, part: int = 0) -> dict:
    base_key = jax.random.key(seed)
    key_head, key_data = jax.random.split(base_key)
    part_key = jax.random.fold_in(key_data, part)
    key_hidden, key_labels = jax.random.split(part_key)
    hidden = jax.random.normal(key_hidden, (TOKENS, HIDDEN), jnp.float32)
    w_head = jax.random.normal(key_head, (HIDDEN, VOCAB), jnp.float32) * (2.0 * HIDDEN ** -0.5)
    labels = jax.random.randint(key_labels, (TOKENS,), 0, VOCAB, jnp.int32)
    labels = labels.at[0].set(VOCAB - 1).at[1].set(0)
    return {"hidden": hidden.astype(jnp.bfloat16), "w_head": w_head.astype(jnp.bfloat16), "labels": labels}


def reference(hidden, w_head, labels):
    inv_tokens = 1.0 / TOKENS
    vocab_ids = jnp.arange(VOCAB, dtype=jnp.int32)
    x_blocks = hidden.reshape(TOKENS // ROW_BLOCK, ROW_BLOCK, HIDDEN)
    lab_blocks = labels.reshape(TOKENS // ROW_BLOCK, ROW_BLOCK)

    def row_pass(block):
        x_block, lab_block = block
        logits = jnp.dot(x_block, w_head, preferred_element_type=jnp.float32)
        row_max = jnp.max(logits, axis=1)
        exp_rows = jnp.exp(logits - row_max[:, None])
        row_sum = jnp.sum(exp_rows, axis=1)
        onehot = vocab_ids[None, :] == lab_block[:, None]
        target = jnp.sum(jnp.where(onehot, logits, 0.0), axis=1)
        tok_loss = row_max + jnp.log(row_sum) - target
        prob_rows = exp_rows / row_sum[:, None]
        grad_logits = (jnp.where(onehot, prob_rows - 1.0, prob_rows) * inv_tokens).astype(jnp.bfloat16)
        d_rows = jnp.dot(grad_logits, w_head.T, preferred_element_type=jnp.float32).astype(jnp.bfloat16)
        return tok_loss, row_max, row_sum, d_rows

    tok_loss, row_max, row_sum, d_rows = lax.map(row_pass, (x_blocks, lab_blocks))
    mean_loss = jnp.mean(tok_loss).reshape(1)
    d_hidden = d_rows.reshape(TOKENS, HIDDEN)

    col_width = VOCAB // VOCAB_SPLIT
    row_count = TOKENS // COL_ROWS
    x_cols = hidden.reshape(row_count, COL_ROWS, HIDDEN)
    lab_cols = labels.reshape(row_count, COL_ROWS)
    max_cols = row_max.reshape(row_count, COL_ROWS)
    sum_cols = row_sum.reshape(row_count, COL_ROWS)
    col_ids = jnp.arange(col_width, dtype=jnp.int32)

    def col_pass(col_index):
        col_start = col_index * col_width
        w_cols = lax.dynamic_slice_in_dim(w_head, col_start, col_width, axis=1)

        def row_step(grad_acc, block):
            x_block, lab_block, max_block, sum_block = block
            logits = jnp.dot(x_block, w_cols, preferred_element_type=jnp.float32)
            onehot = (col_ids + col_start)[None, :] == lab_block[:, None]
            prob_rows = jnp.exp(logits - max_block[:, None]) / sum_block[:, None]
            grad_logits = (jnp.where(onehot, prob_rows - 1.0, prob_rows) * inv_tokens).astype(jnp.bfloat16)
            grad_acc = grad_acc + jnp.dot(x_block.T, grad_logits, preferred_element_type=jnp.float32)
            return grad_acc, None

        grad_init = jnp.zeros((HIDDEN, col_width), jnp.float32)
        grad_acc, unused_out = lax.scan(row_step, grad_init, (x_cols, lab_cols, max_cols, sum_cols))
        return grad_acc.astype(jnp.bfloat16)

    d_blocks = lax.map(col_pass, jnp.arange(VOCAB_SPLIT, dtype=jnp.int32))
    d_w_head = jnp.transpose(d_blocks, (1, 0, 2)).reshape(HIDDEN, VOCAB)
    return mean_loss, d_hidden, d_w_head
```

```python
import jax
import jax.numpy as jnp
from jax import lax
from jax.experimental import pallas as pl
from jax.experimental.pallas import tpu as pltpu
from jax.sharding import PartitionSpec as P


CHUNKS = (384, 1152, 2560, 2560, 2560, 2560, 2560, 1312, 384)
SWAP = [(0, 1), (1, 0)]


def _place_body(start_ref, *refs):
    piece, out, sem = refs[-3], refs[-2], refs[-1]
    rows = piece.shape[0]
    start = pl.multiple_of(start_ref[0] + pl.program_id(0) * rows, 16)
    copy = pltpu.make_async_copy(piece, out.at[pl.ds(start, rows)], sem)
    copy.start()
    copy.wait()


def place(out, piece, start, shape, rows):
    n, cols = piece.shape
    in_specs = [pl.BlockSpec((rows, cols), lambda i, start: (i, 0))]
    args = [piece]
    aliases = {}
    if out is not None:
        in_specs = [pl.BlockSpec(memory_space=pl.ANY)] + in_specs
        args = [out, piece]
        aliases = {1: 0}
    return pl.pallas_call(
        _place_body,
        out_shape=jax.ShapeDtypeStruct(shape, piece.dtype),
        grid_spec=pltpu.PrefetchScalarGridSpec(
            num_scalar_prefetch=1,
            grid=(n // rows,),
            in_specs=in_specs,
            out_specs=pl.BlockSpec(memory_space=pl.ANY),
            scratch_shapes=[pltpu.SemaphoreType.DMA],
        ),
        input_output_aliases=aliases,
        cost_estimate=pl.CostEstimate(flops=n * cols * 4, bytes_accessed=4 * n * cols, transcendentals=0),
        name="place",
    )(jnp.reshape(start, (1,)).astype(jnp.int32), *args)


def dot_f32(a, b, contract):
    return lax.dot_general(a, b, (contract, ((), ())), preferred_element_type=jnp.float32)


def solution(mesh):
    fsdp_size = mesh.shape["fsdp"]
    tp_size = mesh.shape["tp"]
    token_spec = P(("dp", "fsdp", "tp"), None)
    label_spec = P(("dp", "fsdp", "tp"))

    def inner(hidden, w_head, labels):
        rows_dev = hidden.shape[0]
        rows_w, vocab_dev = w_head.shape
        half = vocab_dev // 2
        tokens = rows_dev * tp_size * fsdp_size
        inv_tokens = 1.0 / tokens
        f = lax.axis_index("fsdp")
        is0 = f == 0
        n_chunks = len(CHUNKS)
        offs = [sum(CHUNKS[:k]) for k in range(n_chunks)]

        def swap(a):
            return lax.ppermute(a, "fsdp", SWAP)

        def pick(a, b):
            return jnp.where(is0, a, b)

        hid_peer = swap(hidden)
        lab_peer = swap(labels)
        hid2 = jnp.concatenate([pick(hidden, hid_peer), pick(hid_peer, hidden)], axis=0)
        lab2 = jnp.concatenate([pick(labels, lab_peer), pick(lab_peer, labels)], axis=0)
        lab = lax.all_gather(lab2, "tp", axis=0, tiled=True)
        x_full = lax.all_gather(hid2, "tp", axis=0, tiled=True)
        x_lo, x_hi = x_full[:, :rows_w], x_full[:, rows_w:]
        x_own, x_oth = pick(x_lo, x_hi), pick(x_hi, x_lo)

        wt = w_head.T
        oth = []
        for k, width in enumerate(CHUNKS):
            lo, hi = wt[offs[k] : offs[k] + width], wt[half + offs[k] : half + offs[k] + width]
            oth.append(swap(pick(hi, lo)))
        own = pick(wt[:half], wt[half:])

        ids0 = lab - lax.axis_index("tp") * vocab_dev - f * half

        def onehot(off, width):
            return (ids0 - off)[None, :] == jnp.arange(width, dtype=jnp.int32)[:, None]

        z_own = dot_f32(own, x_own, ((1,), (1,)))
        zs, m, s, t = [], None, None, None
        for k, width in enumerate(CHUNKS):
            head = oth[k]
            if k > 0:
                head, s, t = lax.optimization_barrier((head, s, t))
            z = z_own[offs[k] : offs[k] + width] + dot_f32(head, x_oth, ((1,), (1,)))
            z_max = jnp.max(z, axis=0)
            m_new = z_max if m is None else jnp.maximum(m, z_max)
            s_new = jnp.sum(jnp.exp(z - m_new[None, :]), axis=0)
            t_new = jnp.sum(jnp.where(onehot(offs[k], width), z, 0.0), axis=0)
            s = s_new if m is None else s * jnp.exp(m - m_new) + s_new
            t = t_new if m is None else t + t_new
            m = m_new
            zs.append(z)
        stats = lax.all_gather(jnp.stack([m, s, t]), ("fsdp", "tp"), axis=0)
        row_max = jnp.max(stats[:, 0], axis=0)
        row_sum = jnp.sum(stats[:, 1] * jnp.exp(stats[:, 0] - row_max[None, :]), axis=0)
        target = jnp.sum(stats[:, 2], axis=0)
        tok_loss = row_max + jnp.log(row_sum) - target
        mean_loss = jnp.sum(tok_loss) * inv_tokens

        gs, recv, part = [], [], None
        for k, width in enumerate(CHUNKS):
            z = zs[k]
            if part is not None:
                z, _ = lax.optimization_barrier((z, part))
            prob = jnp.exp(z - row_max[None, :]) / row_sum[None, :]
            g = (jnp.where(onehot(offs[k], width), prob - 1.0, prob) * inv_tokens).astype(jnp.bfloat16)
            part = dot_f32(g, x_oth, ((1,), (0,))).astype(jnp.bfloat16)
            recv.append(swap(part))
            gs.append(g)

        gs, oth, _ = lax.optimization_barrier((gs, oth, part))
        g_all = jnp.concatenate(gs, axis=0)
        oth_all = jnp.concatenate(oth, axis=0)
        dx_own = dot_f32(g_all, own, ((0,), (0,)))
        rs_own = lax.psum_scatter(dx_own, "tp", scatter_dimension=0, tiled=True)
        dx_oth = dot_f32(g_all, oth_all, ((0,), (0,)))
        rs_oth = lax.psum_scatter(dx_oth, "tp", scatter_dimension=0, tiled=True)
        dw_own = dot_f32(g_all, x_own, ((1,), (0,))).astype(jnp.bfloat16)

        def mine(a):
            return pick(a[:rows_dev], a[rows_dev:])

        def theirs(a):
            return pick(a[rows_dev:], a[:rows_dev])

        back_own = swap(theirs(rs_own))
        back_oth = swap(theirs(rs_oth))
        d_own = mine(rs_own) + back_oth
        d_oth = mine(rs_oth) + back_own
        d_hidden = jnp.concatenate([pick(d_own, d_oth), pick(d_oth, d_own)], axis=1).astype(jnp.bfloat16)

        shape = (vocab_dev, rows_w)
        out = place(None, dw_own, f * half, shape, half // 6)
        for k, width in enumerate(CHUNKS):
            rows = width if width <= 512 else width // 2
            out = place(out, recv[k], (1 - f) * half + offs[k], shape, rows)
        return mean_loss.reshape(1), d_hidden, out.T

    return jax.shard_map(
        inner,
        mesh=mesh,
        in_specs=(token_spec, P("fsdp", "tp"), label_spec),
        out_specs=(P("dp"), token_spec, P(("dp", "fsdp"), "tp")),
        check_vma=False,
    )
```

```python
import functools

import jax
import jax.numpy as jnp
from jax import lax
from jax.experimental import pallas as pl
from jax.experimental.layout import Layout, with_layout_constraint
from jax.experimental.pallas import tpu as pltpu
from jax.sharding import PartitionSpec as P


CHUNKS = (256, 1408, 2560, 2560, 2560, 2560, 2560, 1312, 256)
SWAP = [(0, 1), (1, 0)]
SWAP_X = [(0, 2), (2, 0), (1, 3), (3, 1)]
SWAP_CORE = [(0, 1), (1, 0), (2, 3), (3, 2)]


def _place_body(start_ref, *refs):
    piece, out, sem = refs[-3], refs[-2], refs[-1]
    rows = piece.shape[0]
    start = pl.multiple_of(start_ref[0] + pl.program_id(0) * rows, 16)
    copy = pltpu.make_async_copy(piece, out.at[pl.ds(start, rows)], sem)
    copy.start()
    copy.wait()


def place(out, piece, start, shape, rows):
    n, cols = piece.shape
    in_specs = [pl.BlockSpec((rows, cols), lambda i, start: (i, 0))]
    args = [piece]
    aliases = {}
    if out is not None:
        in_specs = [pl.BlockSpec(memory_space=pl.ANY)] + in_specs
        args = [out, piece]
        aliases = {1: 0}
    return pl.pallas_call(
        _place_body,
        out_shape=jax.ShapeDtypeStruct(shape, piece.dtype),
        grid_spec=pltpu.PrefetchScalarGridSpec(
            num_scalar_prefetch=1,
            grid=(n // rows,),
            in_specs=in_specs,
            out_specs=pl.BlockSpec(memory_space=pl.ANY),
            scratch_shapes=[pltpu.SemaphoreType.DMA],
        ),
        input_output_aliases=aliases,
        cost_estimate=pl.CostEstimate(flops=n * cols * 4, bytes_accessed=4 * n * cols, transcendentals=0),
        name="place",
    )(jnp.reshape(start, (1,)).astype(jnp.int32), *args)


def _stats_body(n_f, n_t, mine, res, slots, send_sems, recv_sems):
    dp, f, t = lax.axis_index("dp"), lax.axis_index("fsdp"), lax.axis_index("tp")
    me = f * n_t + t
    peers = [
        (dp, lax.rem(f + j // n_t, n_f), lax.rem(t + j % n_t, n_t)) for j in range(1, n_f * n_t)
    ]
    barrier = pltpu.get_barrier_semaphore()
    for peer in peers:
        pl.semaphore_signal(barrier, inc=1, device_id=peer, device_id_type=pl.DeviceIdType.MESH)
    pl.semaphore_wait(barrier, len(peers))
    copies = []
    for j, peer in enumerate(peers):
        copy = pltpu.make_async_remote_copy(
            src_ref=mine,
            dst_ref=slots.at[me],
            send_sem=send_sems.at[j],
            recv_sem=recv_sems.at[j],
            device_id=peer,
            device_id_type=pl.DeviceIdType.MESH,
        )
        copy.start()
        copies.append(copy)
    slots[me] = mine[...]
    for copy in copies:
        copy.wait()
    m = slots[0, 0:1]
    for d in range(1, n_f * n_t):
        m = jnp.maximum(m, slots[d, 0:1])
    s, t_sum = jnp.zeros_like(m), jnp.zeros_like(m)
    for d in range(n_f * n_t):
        s += slots[d, 1:2] * jnp.exp(slots[d, 0:1] - m)
        t_sum += slots[d, 2:3]
    res[0:1] = m
    res[1:2] = s
    res[2:3] = t_sum


def combine_stats(mine, n_f, n_t):
    n = n_f * n_t
    return pl.pallas_call(
        functools.partial(_stats_body, n_f, n_t),
        out_shape=jax.ShapeDtypeStruct(mine.shape, mine.dtype),
        in_specs=[pl.BlockSpec(memory_space=pltpu.VMEM)],
        out_specs=pl.BlockSpec(memory_space=pltpu.VMEM),
        scratch_shapes=[
            pltpu.VMEM((n,) + mine.shape, mine.dtype),
            pltpu.SemaphoreType.DMA((n - 1,)),
            pltpu.SemaphoreType.DMA((n - 1,)),
        ],
        compiler_params=pltpu.CompilerParams(
            collective_id=0, has_side_effects=True, vmem_limit_bytes=4 * 2**20
        ),
        cost_estimate=pl.CostEstimate(flops=mine.size * 64, bytes_accessed=mine.size * 64, transcendentals=0),
        name="stats",
    )(mine)


def row_major(a):
    return with_layout_constraint(a, Layout(major_to_minor=(0, 1)))


def dot_f32(a, b, contract):
    return lax.dot_general(a, b, (contract, ((), ())), preferred_element_type=jnp.float32)


def solution(mesh):
    fsdp_size = mesh.shape["fsdp"]
    tp_size = mesh.shape["tp"]
    token_spec = P(("dp", "fsdp", "tp"), None)
    label_spec = P(("dp", "fsdp", "tp"))

    def inner(hidden, w_head, labels):
        rows_dev = hidden.shape[0]
        rows_w, vocab_dev = w_head.shape
        half = vocab_dev // 2
        tokens = rows_dev * tp_size * fsdp_size
        inv_tokens = 1.0 / tokens
        f = lax.axis_index("fsdp")
        is0 = f == 0
        n_chunks = len(CHUNKS)
        offs = [sum(CHUNKS[:k]) for k in range(n_chunks)]

        def swap(a):
            return lax.ppermute(a, "fsdp", SWAP)

        def pick(a, b):
            return jnp.where(is0, a, b)

        tp_id = lax.axis_index("tp")

        def pick_x(a, b):
            return jnp.where(tp_id < 2, a, b)

        def pick_c(a, b):
            return jnp.where(tp_id % 2 == 0, a, b)

        def scatter(a):
            half_rows = a.shape[0] // 2
            lo, hi = a[:half_rows], a[half_rows:]
            got = lax.ppermute(pick_c(hi, lo), "tp", SWAP_CORE)
            a = pick_c(lo, hi) + got
            lo, hi = a[: half_rows // 2], a[half_rows // 2 :]
            got = lax.ppermute(pick_x(hi, lo), "tp", SWAP_X)
            return pick_x(lo, hi) + got

        hid_peer = swap(hidden)
        lab_peer = swap(labels)
        hid2 = jnp.concatenate([pick(hidden, hid_peer), pick(hid_peer, hidden)], axis=0)
        lab2 = jnp.concatenate([pick(labels, lab_peer), pick(lab_peer, labels)], axis=0)
        hid_x = lax.ppermute(hid2, "tp", SWAP_X)
        hid4 = jnp.concatenate([pick_x(hid2, hid_x), pick_x(hid_x, hid2)], axis=0)
        hid_c = lax.ppermute(hid4, "tp", SWAP_CORE)
        x_full = jnp.concatenate([pick_c(hid4, hid_c), pick_c(hid_c, hid4)], axis=0)
        lab = lax.all_gather(lab2, "tp", axis=0, tiled=True)
        lab = lab.reshape(2, 2, -1).transpose(1, 0, 2).reshape(-1)
        x_lo, x_hi = x_full[:, :rows_w], x_full[:, rows_w:]
        x_own, x_oth = pick(x_lo, x_hi), pick(x_hi, x_lo)

        wt = row_major(w_head.T)
        oth = []
        for k, width in enumerate(CHUNKS):
            lo, hi = wt[offs[k] : offs[k] + width], wt[half + offs[k] : half + offs[k] + width]
            oth.append(row_major(swap(row_major(pick(hi, lo)))))
        own = pick(wt[:half], wt[half:])

        ids0 = lab - lax.axis_index("tp") * vocab_dev - f * half

        def onehot(off, width):
            return (ids0 - off)[None, :] == jnp.arange(width, dtype=jnp.int32)[:, None]

        z_own = dot_f32(own, x_own, ((1,), (1,)))
        zs, m, s, t = [], None, None, None
        for k, width in enumerate(CHUNKS):
            head = oth[k]
            if k > 0:
                head, s, t = lax.optimization_barrier((head, s, t))
            z = z_own[offs[k] : offs[k] + width] + dot_f32(head, x_oth, ((1,), (1,)))
            z_max = jnp.max(z, axis=0)
            m_new = z_max if m is None else jnp.maximum(m, z_max)
            s_new = jnp.sum(jnp.exp(z - m_new[None, :]), axis=0)
            t_new = jnp.sum(jnp.where(onehot(offs[k], width), z, 0.0), axis=0)
            s = s_new if m is None else s * jnp.exp(m - m_new) + s_new
            t = t_new if m is None else t + t_new
            m = m_new
            zs.append(z)
        stats = combine_stats(jnp.stack([m, s, t]), fsdp_size, tp_size)
        row_max, row_sum, target = stats[0], stats[1], stats[2]
        tok_loss = row_max + jnp.log(row_sum) - target
        mean_loss = jnp.sum(tok_loss) * inv_tokens

        gs, recv, part = [], [], None
        for k, width in enumerate(CHUNKS):
            z = zs[k]
            if part is not None:
                z, _ = lax.optimization_barrier((z, part))
            prob = jnp.exp(z - row_max[None, :]) / row_sum[None, :]
            g = (jnp.where(onehot(offs[k], width), prob - 1.0, prob) * inv_tokens).astype(jnp.bfloat16)
            part = dot_f32(g, x_oth, ((1,), (0,))).astype(jnp.bfloat16)
            recv.append(swap(part))
            gs.append(g)

        gs, oth, _ = lax.optimization_barrier((gs, oth, part))
        g_all = jnp.concatenate(gs, axis=0)
        oth_all = jnp.concatenate(oth, axis=0)
        dx_own = row_major(dot_f32(g_all, own, ((0,), (0,))))
        rs_own = scatter(dx_own)
        dx_oth = row_major(dot_f32(g_all, oth_all, ((0,), (0,))))
        rs_oth = scatter(dx_oth)
        dw_own = dot_f32(g_all, x_own, ((1,), (0,))).astype(jnp.bfloat16)

        def mine(a):
            return pick(a[:rows_dev], a[rows_dev:])

        def theirs(a):
            return pick(a[rows_dev:], a[:rows_dev])

        back_own = swap(theirs(rs_own))
        back_oth = swap(theirs(rs_oth))
        d_own = mine(rs_own) + back_oth
        d_oth = mine(rs_oth) + back_own
        d_hidden = jnp.concatenate([pick(d_own, d_oth), pick(d_oth, d_own)], axis=1).astype(jnp.bfloat16)

        shape = (vocab_dev, rows_w)
        out = place(None, dw_own, f * half, shape, half // 6)
        for k, width in enumerate(CHUNKS):
            rows = width if width <= 512 else width // 2
            out = place(out, recv[k], (1 - f) * half + offs[k], shape, rows)
        return mean_loss.reshape(1), d_hidden, out.T

    return jax.shard_map(
        inner,
        mesh=mesh,
        in_specs=(token_spec, P("fsdp", "tp"), label_spec),
        out_specs=(P("dp"), token_spec, P(("dp", "fsdp"), "tp")),
        check_vma=False,
    )
```
